32 devices in a mesh: leaf: 8 (over z, y), front: 4 (over x, core).
Axes of the slice: x: 2, y: 2, z: 4, core: 2. Of those that a mesh axis runs over, the one named last changes fastest.
Arguments:
- rhs_leaf: float32 [32, 8192], P(None, ('leaf', 'front')), may hold values from -6 to 6
- rhs_sep: float32 [32, 4096], P(None, ('leaf', 'front')), may hold values from -6 to 6
- inv_leaf: float32 [8, 1024, 1024], P('leaf', 'front'), may hold values from -0.1875 to 0.1875
- inv_sep: float32 [8, 512, 512], P('leaf', 'front'), may hold values from -0.25 to 0.25
- push_leaf: float32 [8, 128, 1024], P('leaf', None, 'front'), may hold values from -0.09375 to 0.09375
- push_sep: float32 [8, 128, 512], P('leaf', None, 'front'), may hold values from -0.125 to 0.125
- pull_leaf: float32 [8, 1024, 128], P('leaf', 'front'), may hold values from -0.25 to 0.25
- pull_sep: float32 [8, 512, 128], P('leaf', 'front'), may hold values from -0.25 to 0.25
- rows_leaf: int32 [8, 128], P('leaf'), may hold values from 0 to 511, as said below
- rows_sep: int32 [8, 128], P('leaf'), may hold values from 0 to 511, as said below
- pivot_leaf: int32 [8, 1024], P('leaf'), may hold values from 0 to 1023, each once within a row
- pivot_sep: int32 [8, 512], P('leaf'), may hold values from 0 to 511, each once within a row
- basis_leaf: float32 [50, 8192], P(None, ('leaf', 'front')), may hold values from -6 to 6
- basis_sep: float32 [50, 4096], P(None, ('leaf', 'front')), may hold values from -6 to 6
Outputs:
- q_leaf: float32 [32, 8192], P(None, ('leaf', 'front'))
- q_sep: float32 [32, 4096], P(None, ('leaf', 'front'))
- coeffs: float32 [50, 32], replicated
- rfac: float32 [32, 32], replicated
The draws below stay inside these ranges and needn't reach their ends.
Inputs may be any that keep to these rules, and one draw needn't show every extreme that they name: `rows_leaf`: each row holds 128 different rows of a separator front. `rows_sep`: each row holds 128 different rows of a separator front. `pivot_leaf`: each row is a permutation. `pivot_sep`: each row is a permutation.
All inputs are finite; a program needn't handle non-finite values.
Results may differ from the reference program's by a relative error of at most 0.0001.
Values sent between devices are 32-bit elements; how exact they have to be, the bound alone decides.
No kernel may reach another device: no remote copies, remote signals or barrier semaphores. Data moves between devices by JAX's collectives and lax.ppermute only.
A program may use at most 64 MiB of HBM per device.

```python
import jax
import jax.numpy as jnp
from jax import lax

LEAF_ROWS = 1024
SEP_ROWS = 512
BLOCK = 32
RANK = 50
COUPLE = 128
LEAF_ALL = 8192
SEP_ALL = 4096
N_LEAF = 8


def pick_rows(key):
    scores = jax.random.randint(key, (N_LEAF, SEP_ROWS), 0, 2 ** 18) * SEP_ROWS + jnp.arange(SEP_ROWS, dtype=jnp.int32)[None, :]
    return jnp.argsort(scores, axis=1, stable=True)[:, :COUPLE].astype(jnp.int32)


def draw_rows_leaf(key, part):
    return pick_rows(jax.random.fold_in(key, 101))


def draw_rows_sep(key, part):
    return pick_rows(jax.random.fold_in(key, 202))


def levels(stream_key, shape, pieces, low, largest):
    def one(axis_at, shards_of):
        draws = jax.random.uniform(jax.random.fold_in(jax.random.fold_in(stream_key, 6), axis_at), (shards_of,), jnp.float32, low / len(pieces), largest / len(pieces))
        return jnp.repeat(jnp.exp(draws), shape[axis_at] // shards_of).reshape((-1,) + (1,) * (len(shape) - axis_at - 1))

    level = one(*pieces[0])
    for cut in pieces[1:]:
        level = level * one(*cut)
    return level


def noise(stream_key, dims, width, limit, shards=(), held_as=jnp.bfloat16):
    drawn = width * jax.random.normal(stream_key, dims, jnp.float32)
    if shards:
        drawn = drawn * levels(stream_key, dims, shards, -0.22, 0.18)
    return jnp.clip(drawn, -limit, limit).astype(held_as)


def setup_inputs(seed: int = 0) -> dict:
    streams_of = jax.random.split(jax.random.key(seed), 15)
    return {
        "rhs_leaf": noise(streams_of[0], (BLOCK, LEAF_ALL), 1.0, 6.0, ((1, 32),), jnp.float32),
        "rhs_sep": noise(streams_of[1], (BLOCK, SEP_ALL), 1.0, 6.0, ((1, 32),), jnp.float32),
        "inv_leaf": noise(streams_of[2], (N_LEAF, LEAF_ROWS, LEAF_ROWS), LEAF_ROWS ** -0.5, 0.1875, ((0, 8), (1, 4)), jnp.float32),
        "inv_sep": noise(streams_of[3], (N_LEAF, SEP_ROWS, SEP_ROWS), SEP_ROWS ** -0.5, 0.25, ((0, 8), (1, 4)), jnp.float32),
        "push_leaf": noise(streams_of[4], (N_LEAF, COUPLE, LEAF_ROWS), (4 * LEAF_ROWS) ** -0.5, 0.09375, ((0, 8), (2, 4)), jnp.float32),
        "push_sep": noise(streams_of[5], (N_LEAF, COUPLE, SEP_ROWS), (4 * SEP_ROWS) ** -0.5, 0.125, ((0, 8), (2, 4)), jnp.float32),
        "pull_leaf": noise(streams_of[6], (N_LEAF, LEAF_ROWS, COUPLE), (4 * COUPLE) ** -0.5, 0.25, ((0, 8), (1, 4)), jnp.float32),
        "pull_sep": noise(streams_of[7], (N_LEAF, SEP_ROWS, COUPLE), (4 * COUPLE) ** -0.5, 0.25, ((0, 8), (1, 4)), jnp.float32),
        "rows_leaf": draw_rows_leaf(jax.random.fold_in(streams_of[14], 71), 0),
        "rows_sep": draw_rows_sep(jax.random.fold_in(streams_of[14], 71), 0),
        "pivot_leaf": jax.vmap(lambda own: jax.random.permutation(own, LEAF_ROWS))(jax.random.split(streams_of[10], N_LEAF)).reshape((N_LEAF, LEAF_ROWS)).astype(jnp.int32),
        "pivot_sep": jax.vmap(lambda own: jax.random.permutation(own, SEP_ROWS))(jax.random.split(streams_of[11], N_LEAF)).reshape((N_LEAF, SEP_ROWS)).astype(jnp.int32),
        "basis_leaf": noise(streams_of[12], (RANK, LEAF_ALL), 1.0, 6.0, ((1, 32),), jnp.float32),
        "basis_sep": noise(streams_of[13], (RANK, SEP_ALL), 1.0, 6.0, ((1, 32),), jnp.float32),
    }


exact_mode = lax.Precision.HIGHEST

def contract(former, latter):
    return lax.dot_general(former.astype(jnp.float32), latter.astype(jnp.float32), (((1,), (1,)), ((), ())), precision=exact_mode, preferred_element_type=jnp.float32)

def expand(coeff_block, basis):
    return jnp.dot(coeff_block.T.astype(jnp.float32), basis.astype(jnp.float32), precision=exact_mode, preferred_element_type=jnp.float32)

def apply_inverse(gathered, inverse, pivots):
    return contract(gathered[:, pivots], inverse)

def scatter_rows(partial_term, row_list, sep_width):
    return jnp.zeros((partial_term.shape[0], sep_width), jnp.float32).at[:, row_list].add(partial_term)

def reference(rhs_leaf, rhs_sep, inv_leaf, inv_sep, push_leaf, push_sep, pull_leaf, pull_sep, rows_leaf, rows_sep, pivot_leaf, pivot_sep, basis_leaf, basis_sep):
    groups = N_LEAF
    top_level = groups.bit_length() - 1
    level_of = [top_level + 1] + [(holder & -holder).bit_length() for holder in range(1, groups)]

    def parent_of(holder):
        height = level_of[holder]
        if height == top_level:
            return 0
        return 2 * (holder >> height + 1) + 1 << height
    leaf_rhs = rhs_leaf.reshape(BLOCK, groups, LEAF_ROWS)
    sep_rhs = rhs_sep.reshape(BLOCK, groups, SEP_ROWS)
    leaf_state = [apply_inverse(leaf_rhs[:, holder], inv_leaf[holder], pivot_leaf[holder]) for holder in range(groups)]
    arriving = [jnp.zeros((BLOCK, SEP_ROWS), jnp.float32) for holder in range(groups)]
    for holder in range(groups):
        term = scatter_rows(contract(leaf_state[holder], push_leaf[holder]), rows_leaf[holder], SEP_ROWS)
        arriving[holder | 1] = arriving[holder | 1] + term
    sep_state = [None] * groups
    for height in range(1, top_level + 2):
        for holder in range(groups):
            if level_of[holder] == height:
                sep_state[holder] = apply_inverse(sep_rhs[:, holder] - arriving[holder], inv_sep[holder], pivot_sep[holder])
                if height <= top_level:
                    parent = parent_of(holder)
                    term = scatter_rows(contract(sep_state[holder], push_sep[holder]), rows_sep[holder], SEP_ROWS)
                    arriving[parent] = arriving[parent] + term
    sep_solution = list(sep_state)
    for height in range(top_level, 0, -1):
        for holder in range(groups):
            if level_of[holder] == height:
                above = sep_solution[parent_of(holder)]
                lifted = contract(above[:, rows_sep[holder]], pull_sep[holder])
                sep_solution[holder] = sep_state[holder] - apply_inverse(lifted, inv_sep[holder], pivot_sep[holder])
    leaf_solution = []
    for holder in range(groups):
        lifted = contract(sep_solution[holder | 1][:, rows_leaf[holder]], pull_leaf[holder])
        leaf_solution.append(leaf_state[holder] - apply_inverse(lifted, inv_leaf[holder], pivot_leaf[holder]))
    solved_leaf = jnp.stack(leaf_solution, axis=1).reshape(BLOCK, groups * LEAF_ROWS)
    solved_sep = jnp.stack(sep_solution, axis=1).reshape(BLOCK, groups * SEP_ROWS)
    total_rows = groups * (LEAF_ROWS + SEP_ROWS)
    first_proj = (contract(basis_leaf, solved_leaf) + contract(basis_sep, solved_sep)) / total_rows
    once_leaf = solved_leaf - expand(first_proj, basis_leaf)
    once_sep = solved_sep - expand(first_proj, basis_sep)
    second = (contract(basis_leaf, once_leaf) + contract(basis_sep, once_sep)) / total_rows
    twice_leaf = once_leaf - expand(second, basis_leaf)
    twice_sep = once_sep - expand(second, basis_sep)
    gram_matrix = (contract(twice_leaf, twice_leaf) + contract(twice_sep, twice_sep)) / total_rows
    lower_factor = jnp.linalg.cholesky(gram_matrix)
    q_leaf = lax.linalg.triangular_solve(lower_factor, twice_leaf, left_side=True, lower=True)
    q_sep = lax.linalg.triangular_solve(lower_factor, twice_sep, left_side=True, lower=True)
    return (q_leaf, q_sep, first_proj + second, lower_factor.T)
```

```python
import jax
import jax.numpy as jnp
from jax import lax
from jax.sharding import PartitionSpec as P

exact_mode = lax.Precision.HIGHEST


def mm(former, latter, left=1, right=0):
    return lax.dot_general(
        former,
        latter,
        (((left,), (right,)), ((), ())),
        precision=exact_mode,
        preferred_element_type=jnp.float32,
    )


def swap(value, axis, mask):
    count = lax.axis_size(axis)
    return lax.ppermute(value, axis, [(one, one ^ mask) for one in range(count)])


def gathered_pieces(value, axis):
    return [value] + [swap(value, axis, mask) for mask in range(1, lax.axis_size(axis))]


def doubled_pieces(value, axis):
    count = lax.axis_size(axis)
    pieces = {0: value}
    mask = count // 2
    while mask:
        kept = sorted(pieces)
        moved = swap(jnp.concatenate([pieces[k] for k in kept], 0), axis, mask)
        height = value.shape[0]
        for place, k in enumerate(kept):
            pieces[k ^ mask] = moved[place * height : (place + 1) * height]
        mask //= 2
    return [pieces[k] for k in range(count)]


def summed_pairwise(pieces):
    while len(pieces) > 1:
        pieces = [pieces[k] + pieces[k + 1] for k in range(0, len(pieces), 2)]
    return pieces[0]


def local_place(index, width, own):
    return jnp.bitwise_xor(index // width, own) * width + index % width


def one_hot(places, size):
    return (places[:, None] == lax.broadcasted_iota(jnp.int32, (1, size), 1)).astype(jnp.float32)


def on_device(
    rhs_leaf,
    rhs_sep,
    inv_leaf,
    inv_sep,
    push_leaf,
    push_sep,
    pull_leaf,
    pull_sep,
    rows_leaf,
    rows_sep,
    pivot_leaf,
    pivot_sep,
    basis_leaf,
    basis_sep,
):
    group = lax.axis_index("leaf")
    own = lax.axis_index("front")
    groups = lax.axis_size("leaf")
    top = groups.bit_length() - 1
    leaf_rows = pivot_leaf.shape[1]
    sep_rows = pivot_sep.shape[1]
    leaf_width = rhs_leaf.shape[1]
    sep_width = rhs_sep.shape[1]
    couple = rows_leaf.shape[1]
    total_rows = groups * (leaf_rows + sep_rows)
    level = jnp.full((), top + 1, jnp.int32)
    for bit in range(top, 0, -1):
        level = jnp.where(group % 2**bit != 0, jnp.int32(bit), level)

    leaf_pieces = gathered_pieces(rhs_leaf, "front")
    sep_pieces = gathered_pieces(rhs_sep, "front")
    rhs_leaf_all = jnp.concatenate(leaf_pieces, 1)
    rhs_sep_all = jnp.concatenate(sep_pieces, 1)

    rows_up = jnp.where(level == 1, rows_leaf[0], 0)
    rows_lo = jnp.where(level == 1, swap(rows_leaf, "leaf", 1)[0], 0)
    for height in range(2, top + 2):
        step = 2 ** (height - 2)
        rows_up = jnp.where(level == height, swap(rows_sep, "leaf", step)[0], rows_up)
        if height <= top:
            rows_lo = jnp.where(level == height, swap(rows_sep, "leaf", 3 * step)[0], rows_lo)

    leaf_hot = one_hot(local_place(pivot_leaf[0], leaf_width, own), leaf_rows)
    leaf_map = mm(leaf_hot, inv_leaf[0], 0, 1)
    leaf_state = mm(rhs_leaf_all, leaf_map)
    leaf_push = summed_pairwise(
        gathered_pieces(mm(leaf_state, push_leaf[0], 1, 1), "front")
    )

    bulk = jnp.concatenate([inv_sep[0], push_sep[0].T, pull_sep[0]], 1)
    bulk = jnp.concatenate(doubled_pieces(bulk, "front"), 0)
    sep_inv = bulk[:, :sep_rows]
    push_out = bulk[:, sep_rows : sep_rows + couple]
    pull_all = bulk[:, sep_rows + couple :]
    sep_hot = one_hot(local_place(pivot_sep[0], sep_width, own), sep_rows)
    sep_map = mm(sep_hot, sep_inv, 0, 1)
    lo_hot = one_hot(local_place(rows_lo, sep_width, own), sep_rows)
    up_hot = one_hot(local_place(rows_up, sep_width, own), sep_rows)
    entering = jnp.concatenate([lo_hot, up_hot, pull_all.T, rhs_sep_all], 0)
    leaving = jnp.concatenate([push_out, lo_hot.T, up_hot.T], 1)
    moved = mm(entering, sep_map)
    reduced = mm(moved, leaving)
    up_weights = reduced[: 2 * couple, :couple]
    turn_weights = reduced[: 2 * couple, couple:]
    down_weights = reduced[2 * couple : 3 * couple, couple:]
    push_base = reduced[3 * couple :, :couple]
    row_base = reduced[3 * couple :, couple:]

    pull_leaf_all = jnp.concatenate(doubled_pieces(pull_leaf[0], "front"), 0)
    leaf_lift = mm(pull_leaf_all, leaf_map, 0, 0)

    pair = jnp.concatenate([swap(leaf_push, "leaf", 1), leaf_push], 1)
    pair = jnp.where(level == 1, pair, 0.0)
    for height in range(2, top + 2):
        step = 2 ** (height - 2)
        term = push_base - mm(pair, up_weights)
        upper = swap(term, "leaf", step)
        lower = swap(term, "leaf", 3 * step) if height <= top else jnp.zeros_like(upper)
        pair = jnp.where(level == height, jnp.concatenate([lower, upper], 1), pair)

    row_base = row_base - mm(pair, turn_weights)
    above = jnp.zeros((rhs_leaf.shape[0], couple), jnp.float32)
    for height in range(top + 1, 1, -1):
        step = 2 ** (height - 2)
        below = row_base - mm(above, down_weights)
        upper = swap(below[:, couple:], "leaf", step)
        if height <= top:
            lower = swap(below[:, :couple], "leaf", 3 * step)
            is_upper = (group // (2 * step)) % 2 == 1
            upper = jnp.where(is_upper, upper, lower)
        above = jnp.where(level == height - 1, upper, above)
    below = row_base - mm(above, down_weights)
    leaf_above = jnp.where(level == 1, below[:, couple:], swap(below[:, :couple], "leaf", 1))

    leaf_solution = leaf_state - mm(leaf_above, leaf_lift)
    sep_solution = moved[3 * couple :, :sep_width] - mm(
        jnp.concatenate([pair, above], 1), moved[: 3 * couple, :sep_width]
    )

    basis = jnp.concatenate([basis_leaf, basis_sep], 1)
    solved = jnp.concatenate([leaf_solution, sep_solution], 1)
    metric = mm(basis, basis, 1, 1)
    for axis in ("front", "leaf"):
        mask = 1
        while mask < lax.axis_size(axis):
            metric = metric + swap(metric, axis, mask)
            mask *= 2
    metric = metric / total_rows
    inner = mm(solved, jnp.concatenate([basis, solved], 0), 1, 1)
    inner = summed_pairwise(gathered_pieces(inner, "front"))
    inner = lax.all_to_all(
        jnp.broadcast_to(inner[None], (groups,) + inner.shape), "leaf", 0, 0
    ).sum(0)
    rank = basis.shape[0]
    inner = inner / total_rows
    first = inner[:, :rank]
    second = first - mm(first, metric)
    third = second - mm(second, metric)
    coeffs = first + second
    gram = inner[:, rank:] - mm(
        jnp.concatenate([first, second], 1),
        jnp.concatenate([coeffs, second + third], 1),
        1,
        1,
    )
    lower_factor = jnp.linalg.cholesky(gram, symmetrize_input=True)
    twice = solved - mm(coeffs, basis)
    scaled = lax.linalg.triangular_solve(lower_factor, twice, left_side=True, lower=True)
    return (
        scaled[:, :leaf_width],
        scaled[:, leaf_width:],
        coeffs.T,
        lower_factor.T,
    )


def solution(mesh):
    placed = (
        P(None, ("leaf", "front")),
        P(None, ("leaf", "front")),
        P("leaf", "front", None),
        P("leaf", "front", None),
        P("leaf", None, "front"),
        P("leaf", None, "front"),
        P("leaf", "front", None),
        P("leaf", "front", None),
        P("leaf", None),
        P("leaf", None),
        P("leaf", None),
        P("leaf", None),
        P(None, ("leaf", "front")),
        P(None, ("leaf", "front")),
    )
    return jax.shard_map(
        on_device,
        mesh=mesh,
        in_specs=placed,
        out_specs=(P(None, ("leaf", "front")), P(None, ("leaf", "front")), P(), P()),
        check_vma=False,
    )
```

```python
import jax
import jax.numpy as jnp
from jax import lax
from jax.experimental import pallas as pl
from jax.experimental.pallas import tpu as pltpu
from jax.sharding import PartitionSpec as P


exact_mode = lax.Precision.HIGHEST


def mm(former, latter, left=1, right=0):
    return lax.dot_general(
        former,
        latter,
        (((left,), (right,)), ((), ())),
        precision=exact_mode,
        preferred_element_type=jnp.float32,
    )


def swap(value, axis, mask):
    count = lax.axis_size(axis)
    return lax.ppermute(value, axis, [(one, one ^ mask) for one in range(count)])


def gathered_pieces(value, axis):
    pieces = [value]
    count = lax.axis_size(axis)
    for mask in range(1, count):
        pieces.append(swap(value, axis, mask))
    return pieces


def doubled_pieces(value, axis):
    pieces = {0: value}
    mask = lax.axis_size(axis) // 2
    while mask:
        for k in sorted(pieces):
            pieces[k ^ mask] = swap(pieces[k], axis, mask)
        mask //= 2
    return [pieces[k] for k in sorted(pieces)]


def summed_pairwise(pieces):
    while len(pieces) > 1:
        pieces = [pieces[k] + pieces[k + 1] for k in range(0, len(pieces), 2)]
    return pieces[0]


def local_place(index, width, own):
    return jnp.bitwise_xor(index // width, own) * width + index % width


def one_hot(places, size):
    return (places[:, None] == lax.broadcasted_iota(jnp.int32, (1, size), 1)).astype(jnp.float32)


def pack(inv_ref, push_ref, pull_ref, rhs_ref, out_ref):
    width = push_ref.shape[1]
    place = 0
    for column in range(0, inv_ref.shape[1], width):
        out_ref[place : place + width, :] = inv_ref[:, column : column + width]
        place += width
    for ref in (push_ref, pull_ref, rhs_ref):
        out_ref[place : place + ref.shape[0], :] = ref[...]
        place += ref.shape[0]


def halves(value):
    high = value.astype(jnp.bfloat16)
    rest = value - high.astype(jnp.float32)
    middle = rest.astype(jnp.bfloat16)
    return high, middle, (rest - middle.astype(jnp.float32)).astype(jnp.bfloat16)


def dot(former, latter, left, right):
    return lax.dot_general(
        former, latter, (((left,), (right,)), ((), ())), preferred_element_type=jnp.float32
    )


def reduce_front(members, pivot_ref, rows_ref, *refs):
    pieces = refs[:members]
    moved_ref, up_ref, turn_ref, down_ref, push_base_ref, row_base_ref, root_ref = refs[members:]
    rows = pivot_ref.shape[1]
    width = pieces[0].shape[1]
    couple = rows_ref.shape[1] // 2
    entry = lax.broadcasted_iota(jnp.int32, (rows, rows), 0)
    hot = (entry == pivot_ref[...]).astype(jnp.float32).astype(jnp.bfloat16)
    chosen = (entry[:, : 2 * couple] == rows_ref[...]).astype(jnp.float32).astype(jnp.bfloat16)
    mapped = []
    for piece in pieces:
        inverse = jnp.concatenate(
            [piece[place : place + width, :] for place in range(0, rows, width)], 1
        )
        mapped.append(sum(dot(hot, part, 1, 1) for part in halves(inverse)))
    mapped = jnp.concatenate(mapped, 1)
    push = jnp.concatenate([piece[rows : rows + couple, :] for piece in pieces], 1)
    pull = jnp.concatenate([piece[rows + couple : rows + couple + width, :] for piece in pieces], 0)
    rhs = jnp.concatenate([piece[rows + couple + width :, :] for piece in pieces], 1)
    below = sum(dot(chosen, part, 0, 0) for part in halves(mapped))
    above = mm(pull, mapped, 0, 0)
    base = mm(rhs, mapped, 1, 0)
    moved = jnp.concatenate([below, above, base], 0)
    push_part = mm(moved, push, 1, 1)
    rows_part = sum(dot(part, chosen, 1, 0) for part in halves(moved))
    moved_ref[...] = moved[:, :width]
    up_ref[...] = push_part[: 2 * couple]
    turn_ref[...] = rows_part[: 2 * couple]
    down_ref[...] = rows_part[2 * couple : 3 * couple]
    push_base_ref[...] = push_part[3 * couple :]
    row_base_ref[...] = rows_part[3 * couple :]
    root_ref[:couple, :] = rows_part[couple : 2 * couple, :couple]
    root_ref[couple:, :] = rows_part[3 * couple :, :couple]


def finish(total_rows, inner_ref, leaf_ref, sep_ref, basis_leaf_ref, basis_sep_ref, *outs):
    q_leaf_ref, q_sep_ref, coeffs_ref, rfac_ref = outs
    block = leaf_ref.shape[0]
    rank = basis_leaf_ref.shape[0]
    inner = jnp.sum(inner_ref[...], 0) * (1.0 / total_rows)
    metric = inner[:, :rank]
    first = inner[:, rank : rank + block]
    second = first - mm(metric, first)
    third = second - mm(metric, second)
    coeffs = first + second
    gram = inner[:block, rank + block :] - mm(first, coeffs, 0, 0) - mm(second, second + third, 0, 0)
    coeffs_ref[...] = coeffs.T
    row = lax.broadcasted_iota(jnp.int32, (block, 2 * block), 0)
    lane = lax.broadcasted_iota(jnp.int32, (block, 2 * block), 1)
    table = jnp.concatenate([gram, (row == lane)[:, :block].astype(jnp.float32)], 1)
    pivots = jnp.ones((block, 2 * block), jnp.float32)
    width = 8
    for start in range(0, block, width):
        columns = [
            jnp.broadcast_to(table[:, k : k + 1], table.shape)
            for k in range(start, min(start + width, block))
        ]
        for place in range(len(columns)):
            k = start + place
            pivot = columns[place][k : k + 1, :]
            pivots = jnp.where(row == k, pivot, pivots)
            factor = jnp.where(row > k, columns[place] / pivot, 0.0)
            table = table - factor * table[k : k + 1, :]
            for later in range(place + 1, len(columns)):
                columns[later] = columns[later] - factor * columns[later][k : k + 1, :]
    table = table / jnp.sqrt(pivots)
    rfac_ref[...] = jnp.where(row <= lane, table, 0.0)[:, :block]
    back = table[:, block:]
    spread = mm(back, coeffs, 1, 1)
    q_leaf_ref[...] = mm(back, leaf_ref[...]) - mm(spread, basis_leaf_ref[...])
    q_sep_ref[...] = mm(back, sep_ref[...]) - mm(spread, basis_sep_ref[...])


def on_device(
    rhs_leaf,
    rhs_sep,
    inv_leaf,
    inv_sep,
    push_leaf,
    push_sep,
    pull_leaf,
    pull_sep,
    rows_leaf,
    rows_sep,
    pivot_leaf,
    pivot_sep,
    basis_leaf,
    basis_sep,
):
    group = lax.axis_index("leaf")
    own = lax.axis_index("front")
    groups = lax.axis_size("leaf")
    top = groups.bit_length() - 1
    leaf_rows = pivot_leaf.shape[1]
    sep_rows = pivot_sep.shape[1]
    leaf_width = rhs_leaf.shape[1]
    sep_width = rhs_sep.shape[1]
    couple = rows_leaf.shape[1]
    total_rows = groups * (leaf_rows + sep_rows)
    level = jnp.full((), top + 1, jnp.int32)
    for bit in range(top, 0, -1):
        level = jnp.where(group % 2**bit != 0, jnp.int32(bit), level)

    rhs_leaf_all = jnp.concatenate(gathered_pieces(rhs_leaf, "front"), 1)
    bulk = pl.pallas_call(
        pack,
        out_shape=jax.ShapeDtypeStruct(
            (sep_rows + 2 * couple + rhs_sep.shape[0], sep_width), jnp.float32
        ),
        name="pack",
    )(inv_sep[0], push_sep[0], pull_sep[0], rhs_sep)
    bulk = doubled_pieces(bulk, "front")

    lists = jnp.concatenate([rows_leaf, rows_sep], 0)
    lists = lax.all_to_all(
        jnp.broadcast_to(lists[None], (groups,) + lists.shape), "leaf", 0, 0
    )
    reach = jnp.where(level == 1, 0, jnp.left_shift(1, jnp.maximum(level - 2, 0)))
    upper_child = group + reach
    lower_child = jnp.where(level == 1, group - 1, jnp.where(level > top, reach, group - reach))
    kind = jnp.where(level == 1, 0, 1)
    rows = jnp.concatenate(
        [
            lax.dynamic_slice(lists, (child, kind, 0), (1, 1, couple))[0]
            for child in (lower_child, upper_child)
        ],
        1,
    )

    leaf_hot = one_hot(local_place(pivot_leaf[0], leaf_width, own), leaf_rows)
    leaf_map = mm(leaf_hot, inv_leaf[0], 0, 1)
    leaf_state = mm(rhs_leaf_all, leaf_map)
    leaf_push = summed_pairwise(
        gathered_pieces(mm(leaf_state, push_leaf[0], 1, 1), "front")
    )

    vmem = pl.BlockSpec(memory_space=pltpu.VMEM)
    block = rhs_sep.shape[0]
    shapes = (
        (3 * couple + block, sep_width),
        (2 * couple, couple),
        (2 * couple, 2 * couple),
        (couple, 2 * couple),
        (block, couple),
        (block, 2 * couple),
        (couple + block, couple),
    )
    moved, up_weights, turn_weights, down_weights, push_base, row_base, root_op = pl.pallas_call(
        lambda *refs: reduce_front(len(bulk), *refs),
        out_shape=tuple(jax.ShapeDtypeStruct(shape, jnp.float32) for shape in shapes),
        out_specs=(vmem,) * len(shapes),
        name="reduce_front",
    )(
        local_place(pivot_sep, sep_width, own),
        local_place(rows, sep_width, own),
        *bulk,
    )

    pull_leaf_all = jnp.concatenate(doubled_pieces(pull_leaf[0], "front"), 0)
    leaf_lift = mm(pull_leaf_all, leaf_map, 0, 0)

    half = groups // 2
    root_op = swap(root_op, "leaf", half)

    pair = jnp.concatenate([swap(leaf_push, "leaf", 1), leaf_push], 1)
    pair = jnp.where(level == 1, pair, 0.0)
    for height in range(2, top + 1):
        step = 2 ** (height - 2)
        term = push_base - mm(pair, up_weights)
        upper = swap(term, "leaf", step)
        lower = swap(term, "leaf", 3 * step)
        pair = jnp.where(level == height, jnp.concatenate([lower, upper], 1), pair)

    term = push_base - mm(pair, up_weights)
    above = jnp.where(level == top, root_op[couple:] - mm(term, root_op[:couple]), 0.0)
    back = swap(term, "leaf", half)

    row_base = row_base - mm(pair, turn_weights)
    for height in range(top, 1, -1):
        step = 2 ** (height - 2)
        below = row_base - mm(above, down_weights)
        upper = swap(below[:, couple:], "leaf", step)
        lower = swap(below[:, :couple], "leaf", 3 * step)
        is_upper = (group // (2 * step)) % 2 == 1
        above = jnp.where(level == height - 1, jnp.where(is_upper, upper, lower), above)
    below = row_base - mm(above, down_weights)
    leaf_above = jnp.where(level == 1, below[:, couple:], swap(below[:, :couple], "leaf", 1))
    around = jnp.concatenate([pair, above], 1)
    root_around = jnp.pad(back, ((0, 0), (couple, couple)))
    around = jnp.where(level > top, root_around, around)

    leaf_solution = leaf_state - mm(leaf_above, leaf_lift)
    sep_solution = moved[3 * couple :] - mm(
        around, moved[: 3 * couple]
    )

    rank = basis_leaf.shape[0]
    metric = mm(basis_leaf, basis_leaf, 1, 1) + mm(basis_sep, basis_sep, 1, 1)
    cross = mm(basis_leaf, leaf_solution, 1, 1) + mm(basis_sep, sep_solution, 1, 1)
    length = mm(leaf_solution, leaf_solution, 1, 1) + mm(sep_solution, sep_solution, 1, 1)
    inner = jnp.concatenate([metric, cross, jnp.pad(length, ((0, rank - block), (0, 0)))], 1)
    inner = summed_pairwise(gathered_pieces(inner, "front"))
    inner = lax.all_to_all(
        jnp.broadcast_to(inner[None], (groups,) + inner.shape), "leaf", 0, 0
    )
    q_leaf, q_sep, coeffs, rfac = pl.pallas_call(
        lambda *refs: finish(total_rows, *refs),
        out_shape=(
            jax.ShapeDtypeStruct((block, leaf_width), jnp.float32),
            jax.ShapeDtypeStruct((block, sep_width), jnp.float32),
            jax.ShapeDtypeStruct((block, rank), jnp.float32),
            jax.ShapeDtypeStruct((block, block), jnp.float32),
        ),
        name="finish",
    )(inner, leaf_solution, sep_solution, basis_leaf, basis_sep)
    return q_leaf, q_sep, coeffs.T, rfac


def solution(mesh):
    placed = (
        P(None, ("leaf", "front")),
        P(None, ("leaf", "front")),
        P("leaf", "front", None),
        P("leaf", "front", None),
        P("leaf", None, "front"),
        P("leaf", None, "front"),
        P("leaf", "front", None),
        P("leaf", "front", None),
        P("leaf", None),
        P("leaf", None),
        P("leaf", None),
        P("leaf", None),
        P(None, ("leaf", "front")),
        P(None, ("leaf", "front")),
    )

    return jax.shard_map(
        on_device,
        mesh=mesh,
        in_specs=placed,
        out_specs=(P(None, ("leaf", "front")), P(None, ("leaf", "front")), P(), P()),
        check_vma=False,
    )
```

```python
import jax
import jax.numpy as jnp
from jax import lax
from jax.experimental import pallas as pl
from jax.experimental.pallas import tpu as pltpu
from jax.sharding import PartitionSpec as P


exact_mode = lax.Precision.HIGHEST


def mm(former, latter, left=1, right=0):
    return lax.dot_general(
        former,
        latter,
        (((left,), (right,)), ((), ())),
        precision=exact_mode,
        preferred_element_type=jnp.float32,
    )


def swap(value, axis, mask):
    count = lax.axis_size(axis)
    return lax.ppermute(value, axis, [(one, one ^ mask) for one in range(count)])


def gathered_pieces(value, axis):
    pieces = [value]
    count = lax.axis_size(axis)
    for mask in range(1, count):
        pieces.append(swap(value, axis, mask))
    return pieces


def doubled_pieces(value, axis):
    pieces = {0: value}
    mask = lax.axis_size(axis) // 2
    while mask:
        for k in sorted(pieces):
            pieces[k ^ mask] = swap(pieces[k], axis, mask)
        mask //= 2
    return [pieces[k] for k in sorted(pieces)]


def summed_pairwise(pieces):
    while len(pieces) > 1:
        pieces = [pieces[k] + pieces[k + 1] for k in range(0, len(pieces), 2)]
    return pieces[0]


def local_place(index, width, own):
    if width & (width - 1) == 0:
        return jnp.bitwise_xor(index, own * width)
    return jnp.bitwise_xor(index // width, own) * width + index % width


def level_of(group, top):
    level = jnp.int32(top + 1)
    for bit in range(top, 0, -1):
        level = jnp.where(group % 2**bit != 0, jnp.int32(bit), level)
    return level


def held(arrays):
    return [pltpu.with_memory_space_constraint(array, pltpu.VMEM) for array in arrays]


def pack(inv_ref, push_ref, pull_ref, rhs_ref, out_ref):
    width = push_ref.shape[1]
    place = 0
    for column in range(0, inv_ref.shape[1], width):
        out_ref[place : place + width, :] = inv_ref[:, column : column + width]
        place += width
    for ref in (push_ref, pull_ref, rhs_ref):
        out_ref[place : place + ref.shape[0], :] = ref[...]
        place += ref.shape[0]


def halves(value):
    high = value.astype(jnp.bfloat16)
    rest = value - high.astype(jnp.float32)
    middle = rest.astype(jnp.bfloat16)
    return high, middle, (rest - middle.astype(jnp.float32)).astype(jnp.bfloat16)


def dot(former, latter, left, right):
    return lax.dot_general(
        former, latter, (((left,), (right,)), ((), ())), preferred_element_type=jnp.float32
    )


def permuting(pivot_ref, width):
    rows = pivot_ref.shape[1]
    places = local_place(pivot_ref[...], width, lax.axis_index("front"))
    entry = lax.broadcasted_iota(jnp.int32, (rows, rows), 0)
    return (entry == places).astype(jnp.float32).astype(jnp.bfloat16)


def solve_leaf(pivot_ref, inv_ref, push_ref, *refs):
    pieces, (state_ref, term_ref) = refs[:-2], refs[-2:]
    hot = permuting(pivot_ref, pieces[0].shape[1])
    rhs = jnp.concatenate([piece[...] for piece in pieces], 1)
    block = rhs.shape[0]
    turned = dot(jnp.concatenate(halves(rhs), 0), hot, 1, 0)
    turned = turned[:block] + turned[block : 2 * block] + turned[2 * block :]
    state = mm(turned, inv_ref[...], 1, 1)
    state_ref[...] = state
    term_ref[...] = mm(state, push_ref[...], 1, 1)


def turn_pull(pivot_ref, *refs):
    pieces, turned_ref = refs[:-1], refs[-1]
    hot = permuting(pivot_ref, pieces[0].shape[0])
    pull = jnp.concatenate([piece[...] for piece in pieces], 0).T
    couple = pull.shape[0]
    turned = dot(jnp.concatenate(halves(pull), 0), hot, 1, 0)
    turned_ref[...] = turned[:couple] + turned[couple : 2 * couple] + turned[2 * couple :]


def reduce_front(top, pivot_ref, lists_ref, *refs):
    pieces = refs[:-8]
    below_ref, rest_ref, up_ref, turn_ref, down_ref, push_base_ref, row_base_ref, root_ref = refs[-8:]
    rows = pivot_ref.shape[1]
    width = pieces[0].shape[1]
    couple = lists_ref.shape[1]
    hot = permuting(pivot_ref, width)
    group = lax.axis_index("leaf")
    level = level_of(group, top)
    reach = jnp.where(level == 1, 0, jnp.left_shift(1, jnp.maximum(level - 2, 0)))
    lower = jnp.where(level == 1, group - 1, jnp.where(level > top, reach, group - reach))
    kind = jnp.where(level == 1, 0, 1)
    children = jnp.concatenate(
        [lists_ref[pl.ds(2 * child + kind, 1), :] for child in (lower, group + reach)], 1
    )
    children = local_place(children, width, lax.axis_index("front"))
    entry = lax.broadcasted_iota(jnp.int32, (rows, 2 * couple), 0)
    chosen = (entry == children).astype(jnp.float32).astype(jnp.bfloat16)
    mapped = []
    for piece in pieces:
        inverse = jnp.concatenate(
            [piece[place : place + width, :] for place in range(0, rows, width)], 1
        )
        mapped.append(sum(dot(hot, part, 1, 1) for part in halves(inverse)))
    mapped = jnp.concatenate(mapped, 1)
    push = jnp.concatenate([piece[rows : rows + couple, :] for piece in pieces], 1)
    pull = jnp.concatenate([piece[rows + couple : rows + couple + width, :] for piece in pieces], 0)
    rhs = jnp.concatenate([piece[rows + couple + width :, :] for piece in pieces], 1)
    below = sum(dot(chosen, part, 0, 0) for part in halves(mapped))
    moved = jnp.concatenate([below, mm(jnp.concatenate([pull.T, rhs], 0), mapped)], 0)
    push_part = mm(moved, push, 1, 1)
    rows_part = sum(dot(part, chosen, 1, 0) for part in halves(moved))
    below_ref[...] = moved[: 2 * couple, :width]
    rest_ref[...] = moved[2 * couple :, :width]
    up_ref[...] = push_part[: 2 * couple]
    turn_ref[...] = rows_part[: 2 * couple]
    down_ref[...] = rows_part[2 * couple : 3 * couple]
    push_base_ref[...] = push_part[3 * couple :]
    row_base_ref[...] = rows_part[3 * couple :]
    root_ref[:couple, :] = rows_part[couple : 2 * couple, :couple]
    root_ref[couple:, :] = rows_part[3 * couple :, :couple]


def project(top, *refs):
    state_ref, below_ref, moved_in_ref, lift_ref, pair_ref, above_ref, back_ref = refs[:7]
    below_map_ref, rest_ref, metric_ref, basis_leaf_ref, basis_sep_ref = refs[7:12]
    leaf_ref, sep_ref, inner_ref = refs[12:]
    couple = moved_in_ref.shape[1]
    block = state_ref.shape[0]
    rank = basis_leaf_ref.shape[0]
    level = level_of(lax.axis_index("leaf"), top)
    above = jnp.where(level == 1, below_ref[:, couple:], moved_in_ref[...])
    leaf = state_ref[...] - mm(above, lift_ref[...])
    width = sep_ref.shape[1]
    is_root = level > top
    upper = jnp.where(is_root, back_ref[...], pair_ref[:, couple:])
    around = jnp.concatenate([jnp.where(is_root, 0.0, pair_ref[:, :couple]), upper], 1)
    sep = (
        rest_ref[couple:, :width]
        - mm(around, below_map_ref[...])
        - mm(above_ref[...], rest_ref[:couple, :width])
    )
    leaf_ref[...] = leaf
    sep_ref[...] = sep
    row = lax.broadcasted_iota(jnp.int32, (block, block), 0)
    lane = lax.broadcasted_iota(jnp.int32, (block, block), 1)
    corner = metric_ref[:block, :block]
    length = mm(leaf, leaf, 1, 1) + mm(sep, sep, 1, 1)
    inner_ref[...] = jnp.zeros(inner_ref.shape, jnp.float32)
    inner_ref[:, :rank] = mm(leaf, basis_leaf_ref[...], 1, 1) + mm(sep, basis_sep_ref[...], 1, 1)
    inner_ref[:, rank : rank + block] = jnp.where(row <= lane, length, corner)
    place = rank + block
    inner_ref[:, place : place + 1] = jnp.sum(jnp.where(row == lane, corner, 0.0), 1, keepdims=True)
    rest = rank - block
    inner_ref[:, place + 1 : place + 1 + rest] = metric_ref[:block, block:]
    inner_ref[:rest, place + 1 + rest : place + 1 + 2 * rest] = metric_ref[block:, block:]


def finish(total_rows, inner_ref, leaf_ref, sep_ref, basis_leaf_ref, basis_sep_ref, *outs):
    q_leaf_ref, q_sep_ref, coeffs_ref, rfac_ref = outs
    block = leaf_ref.shape[0]
    rank = basis_leaf_ref.shape[0]
    rest = rank - block
    inner = jnp.sum(inner_ref[...], 0) * (1.0 / total_rows)
    row = lax.broadcasted_iota(jnp.int32, (block, block), 0)
    lane = lax.broadcasted_iota(jnp.int32, (block, block), 1)
    first = inner[:, :rank]
    both = inner[:, rank : rank + block]
    place = rank + block
    length = jnp.where(row <= lane, both, both.T)
    corner = jnp.where(row > lane, both, both.T)
    corner = jnp.where(row == lane, inner[:, place : place + 1], corner)
    side = inner[:, place + 1 : place + 1 + rest]
    last = inner[:rest, place + 1 + rest : place + 1 + 2 * rest]

    def by_metric(value):
        low, high = value[:, :block], value[:, block:]
        return jnp.concatenate(
            [mm(low, corner) + mm(high, side, 1, 1), mm(low, side) + mm(high, last)], 1
        )

    second = first - by_metric(first)
    third = second - by_metric(second)
    coeffs = first + second
    gram = length - mm(first, coeffs, 1, 1) - mm(second, second + third, 1, 1)
    coeffs_ref[...] = coeffs
    row = lax.broadcasted_iota(jnp.int32, (block, 2 * block), 0)
    lane = lax.broadcasted_iota(jnp.int32, (block, 2 * block), 1)
    table = jnp.concatenate([gram, (row == lane)[:, :block].astype(jnp.float32)], 1)
    pivots = jnp.ones((block, 2 * block), jnp.float32)
    width = 8
    for start in range(0, block, width):
        columns = [
            jnp.broadcast_to(table[:, k : k + 1], table.shape)
            for k in range(start, min(start + width, block))
        ]
        for place in range(len(columns)):
            k = start + place
            pivot = columns[place][k : k + 1, :]
            pivots = jnp.where(row == k, pivot, pivots)
            factor = jnp.where(row > k, columns[place] / pivot, 0.0)
            table = table - factor * table[k : k + 1, :]
            for later in range(place + 1, len(columns)):
                columns[later] = columns[later] - factor * columns[later][k : k + 1, :]
    table = table / jnp.sqrt(pivots)
    rfac_ref[...] = jnp.where(row <= lane, table, 0.0)[:, :block]
    back = table[:, block:]
    spread = mm(back, coeffs)
    q_leaf_ref[...] = mm(back, leaf_ref[...]) - mm(spread, basis_leaf_ref[...])
    q_sep_ref[...] = mm(back, sep_ref[...]) - mm(spread, basis_sep_ref[...])


def on_device(
    rhs_leaf,
    rhs_sep,
    inv_leaf,
    inv_sep,
    push_leaf,
    push_sep,
    pull_leaf,
    pull_sep,
    rows_leaf,
    rows_sep,
    pivot_leaf,
    pivot_sep,
    basis_leaf,
    basis_sep,
):
    group = lax.axis_index("leaf")
    groups = lax.axis_size("leaf")
    top = groups.bit_length() - 1
    leaf_rows = pivot_leaf.shape[1]
    sep_rows = pivot_sep.shape[1]
    leaf_width = rhs_leaf.shape[1]
    sep_width = rhs_sep.shape[1]
    couple = rows_leaf.shape[1]
    total_rows = groups * (leaf_rows + sep_rows)
    level = level_of(group, top)

    leaf_pieces = gathered_pieces(rhs_leaf, "front")

    bulk = pl.pallas_call(
        pack,
        out_shape=pltpu.VMEM((sep_rows + 2 * couple + rhs_sep.shape[0], sep_width), jnp.float32),
        in_specs=[pl.BlockSpec(memory_space=pltpu.VMEM)] * 4,
        out_specs=pl.BlockSpec(memory_space=pltpu.VMEM),
        name="pack",
    )(inv_sep[0], push_sep[0], pull_sep[0], rhs_sep)
    bulk = doubled_pieces(bulk, "front")

    lists = jnp.concatenate([rows_leaf, rows_sep], 0)
    lists = lax.all_to_all(
        jnp.broadcast_to(lists[None], (groups,) + lists.shape), "leaf", 0, 0
    )
    vmem = pl.BlockSpec(memory_space=pltpu.VMEM)
    block = rhs_sep.shape[0]
    leaf_state, leaf_push = pl.pallas_call(
        solve_leaf,
        out_shape=(
            pltpu.VMEM((block, leaf_width), jnp.float32),
            pltpu.VMEM((block, couple), jnp.float32),
        ),
        in_specs=[vmem] * (3 + len(leaf_pieces)),
        out_specs=(vmem,) * 2,
        name="solve_leaf",
    )(pivot_leaf, inv_leaf[0], push_leaf[0], leaf_pieces[0], *held(leaf_pieces[1:]))
    leaf_push = summed_pairwise(gathered_pieces(leaf_push, "front"))

    shapes = (
        (2 * couple, sep_width),
        (couple + block, sep_width),
        (2 * couple, couple),
        (2 * couple, 2 * couple),
        (couple, 2 * couple),
        (block, couple),
        (block, 2 * couple),
        (couple + block, couple),
    )
    (
        below_map,
        rest,
        up_weights,
        turn_weights,
        down_weights,
        push_base,
        row_base,
        root_op,
    ) = pl.pallas_call(
        lambda *refs: reduce_front(top, *refs),
        out_shape=tuple(pltpu.VMEM(shape, jnp.float32) for shape in shapes),
        in_specs=[vmem] * (2 + len(bulk)),
        out_specs=(vmem,) * len(shapes),
        name="reduce_front",
    )(pivot_sep, lists.reshape(2 * groups, couple), *bulk)

    pull_pieces = doubled_pieces(pull_leaf[0], "front")
    leaf_turned = pl.pallas_call(
        turn_pull,
        out_shape=pltpu.VMEM((couple, leaf_rows), jnp.float32),
        in_specs=[vmem] * (1 + len(pull_pieces)),
        out_specs=vmem,
        name="turn_pull",
    )(pivot_leaf, pull_pieces[0], *held(pull_pieces[1:]))
    leaf_lift = mm(leaf_turned, inv_leaf[0], 1, 1)

    half = groups // 2
    root_op = swap(root_op, "leaf", half)

    pair = jnp.concatenate([swap(leaf_push, "leaf", 1), leaf_push], 1)
    pair = jnp.where(level == 1, pair, 0.0)
    for height in range(2, top + 1):
        step = 2 ** (height - 2)
        term = push_base - mm(pair, up_weights)
        upper = swap(term, "leaf", step)
        lower = swap(term, "leaf", 3 * step)
        pair = jnp.where(level == height, jnp.concatenate([lower, upper], 1), pair)

    term = push_base - mm(pair, up_weights)
    above = jnp.where(level == top, root_op[couple:] - mm(term, root_op[:couple]), 0.0)
    back = swap(term, "leaf", half)

    row_base = row_base - mm(pair, turn_weights)
    for height in range(top, 1, -1):
        step = 2 ** (height - 2)
        below = row_base - mm(above, down_weights)
        upper = swap(below[:, couple:], "leaf", step)
        lower = swap(below[:, :couple], "leaf", 3 * step)
        is_upper = (group // (2 * step)) % 2 == 1
        above = jnp.where(level == height - 1, jnp.where(is_upper, upper, lower), above)
    below = row_base - mm(above, down_weights)
    moved_in = swap(below[:, :couple], "leaf", 1)
    rank = basis_leaf.shape[0]
    metric = mm(basis_leaf, basis_leaf, 1, 1) + mm(basis_sep, basis_sep, 1, 1)
    lanes = -(-(3 * rank - block + 1) // 128) * 128
    leaf_solution, sep_solution, inner = pl.pallas_call(
        lambda *refs: project(top, *refs),
        out_shape=(
            pltpu.VMEM((block, leaf_width), jnp.float32),
            pltpu.VMEM((block, sep_width), jnp.float32),
            pltpu.VMEM((block, lanes), jnp.float32),
        ),
        in_specs=[vmem] * 12,
        out_specs=(vmem,) * 3,
        name="project",
    )(
        *held([leaf_state, below, moved_in, leaf_lift, pair, above, back, below_map, rest, metric]),
        basis_leaf,
        basis_sep,
    )
    inner = summed_pairwise(gathered_pieces(inner, "front"))
    inner = lax.all_to_all(
        jnp.broadcast_to(inner[None], (groups,) + inner.shape), "leaf", 0, 0
    )
    q_leaf, q_sep, coeffs, rfac = pl.pallas_call(
        lambda *refs: finish(total_rows, *refs),
        out_shape=(
            jax.ShapeDtypeStruct((block, leaf_width), jnp.float32),
            jax.ShapeDtypeStruct((block, sep_width), jnp.float32),
            jax.ShapeDtypeStruct((block, rank), jnp.float32),
            jax.ShapeDtypeStruct((block, block), jnp.float32),
        ),
        in_specs=[vmem] * 5,
        name="finish",
    )(*held([inner, leaf_solution, sep_solution]), basis_leaf, basis_sep)
    return q_leaf, q_sep, coeffs.T, rfac


def solution(mesh):
    placed = (
        P(None, ("leaf", "front")),
        P(None, ("leaf", "front")),
        P("leaf", "front", None),
        P("leaf", "front", None),
        P("leaf", None, "front"),
        P("leaf", None, "front"),
        P("leaf", "front", None),
        P("leaf", "front", None),
        P("leaf", None),
        P("leaf", None),
        P("leaf", None),
        P("leaf", None),
        P(None, ("leaf", "front")),
        P(None, ("leaf", "front")),
    )

    return jax.shard_map(
        on_device,
        mesh=mesh,
        in_specs=placed,
        out_specs=(P(None, ("leaf", "front")), P(None, ("leaf", "front")), P(), P()),
        check_vma=False,
    )
```

```python
import jax
import jax.numpy as jnp
from jax import lax
from jax.experimental import pallas as pl
from jax.experimental.pallas import tpu as pltpu
from jax.sharding import PartitionSpec as P


exact_mode = lax.Precision.HIGHEST


def mm(former, latter, left=1, right=0):
    return lax.dot_general(
        former,
        latter,
        (((left,), (right,)), ((), ())),
        precision=exact_mode,
        preferred_element_type=jnp.float32,
    )


def swap(value, axis, mask):
    count = lax.axis_size(axis)
    return lax.ppermute(value, axis, [(one, one ^ mask) for one in range(count)])


def gathered_pieces(value, axis):
    pieces = [value]
    count = lax.axis_size(axis)
    for mask in range(1, count):
        pieces.append(swap(value, axis, mask))
    return pieces


def doubled_pieces(value, axis):
    pieces = {0: value}
    mask = lax.axis_size(axis) // 2
    while mask:
        for k in sorted(pieces):
            pieces[k ^ mask] = swap(pieces[k], axis, mask)
        mask //= 2
    return [pieces[k] for k in sorted(pieces)]


def summed_pairwise(pieces):
    while len(pieces) > 1:
        pieces = [pieces[k] + pieces[k + 1] for k in range(0, len(pieces), 2)]
    return pieces[0]


def local_place(index, width, own):
    if width & (width - 1) == 0:
        return jnp.bitwise_xor(index, own * width)
    return jnp.bitwise_xor(index // width, own) * width + index % width


def level_of(group, top):
    level = jnp.int32(top + 1)
    for bit in range(top, 0, -1):
        level = jnp.where(group % 2**bit != 0, jnp.int32(bit), level)
    return level


def held(arrays):
    return [pltpu.with_memory_space_constraint(array, pltpu.VMEM) for array in arrays]


def pack(inv_ref, push_ref, pull_ref, rhs_ref, out_ref):
    width = push_ref.shape[1]
    place = 0
    for column in range(0, inv_ref.shape[1], width):
        out_ref[place : place + width, :] = inv_ref[:, column : column + width]
        place += width
    for ref in (push_ref, pull_ref, rhs_ref):
        out_ref[place : place + ref.shape[0], :] = ref[...]
        place += ref.shape[0]


def halves(value):
    high = value.astype(jnp.bfloat16)
    rest = value - high.astype(jnp.float32)
    middle = rest.astype(jnp.bfloat16)
    return high, middle, (rest - middle.astype(jnp.float32)).astype(jnp.bfloat16)


def dot(former, latter, left, right):
    return lax.dot_general(
        former, latter, (((left,), (right,)), ((), ())), preferred_element_type=jnp.float32
    )


def permuting(pivot_ref, width):
    rows = pivot_ref.shape[1]
    places = local_place(pivot_ref[...], width, lax.axis_index("front"))
    entry = lax.broadcasted_iota(jnp.int32, (rows, rows), 0)
    return (entry == places).astype(jnp.float32).astype(jnp.bfloat16)


def solve_leaf(pivot_ref, inv_ref, push_ref, *refs):
    pieces, (state_ref, term_ref) = refs[:-2], refs[-2:]
    hot = permuting(pivot_ref, pieces[0].shape[1])
    rhs = jnp.concatenate([piece[...] for piece in pieces], 1)
    block = rhs.shape[0]
    turned = dot(jnp.concatenate(halves(rhs), 0), hot, 1, 0)
    turned = turned[:block] + turned[block : 2 * block] + turned[2 * block :]
    state = mm(turned, inv_ref[...], 1, 1)
    state_ref[...] = state
    term_ref[...] = mm(state, push_ref[...], 1, 1)


def turn_pull(pivot_ref, *refs):
    pieces, turned_ref = refs[:-1], refs[-1]
    hot = permuting(pivot_ref, pieces[0].shape[0])
    pull = jnp.concatenate([piece[...] for piece in pieces], 0).T
    couple = pull.shape[0]
    turned = dot(jnp.concatenate(halves(pull), 0), hot, 1, 0)
    turned_ref[...] = turned[:couple] + turned[couple : 2 * couple] + turned[2 * couple :]


def reduce_front(top, pivot_ref, lists_ref, *refs):
    pieces = refs[:-8]
    below_ref, rest_ref, up_ref, turn_ref, down_ref, push_base_ref, row_base_ref, root_ref = refs[-8:]
    rows = pivot_ref.shape[1]
    width = pieces[0].shape[1]
    couple = lists_ref.shape[1]
    hot = permuting(pivot_ref, width)
    group = lax.axis_index("leaf")
    level = level_of(group, top)
    reach = jnp.where(level == 1, 0, jnp.left_shift(1, jnp.maximum(level - 2, 0)))
    lower = jnp.where(level == 1, group - 1, jnp.where(level > top, reach, group - reach))
    kind = jnp.where(level == 1, 0, 1)
    children = jnp.concatenate(
        [lists_ref[pl.ds(2 * child + kind, 1), :] for child in (lower, group + reach)], 1
    )
    children = local_place(children, width, lax.axis_index("front"))
    entry = lax.broadcasted_iota(jnp.int32, (rows, 2 * couple), 0)
    chosen = (entry == children).astype(jnp.float32).astype(jnp.bfloat16)
    mapped = []
    for piece in pieces:
        inverse = jnp.concatenate(
            [piece[place : place + width, :] for place in range(0, rows, width)], 1
        )
        mapped.append(sum(dot(hot, part, 1, 1) for part in halves(inverse)))
    mapped = jnp.concatenate(mapped, 1)
    push = jnp.concatenate([piece[rows : rows + couple, :] for piece in pieces], 1)
    pull = jnp.concatenate([piece[rows + couple : rows + couple + width, :] for piece in pieces], 0)
    rhs = jnp.concatenate([piece[rows + couple + width :, :] for piece in pieces], 1)
    below = sum(dot(chosen, part, 0, 0) for part in halves(mapped))
    moved = jnp.concatenate([below, mm(jnp.concatenate([pull.T, rhs], 0), mapped)], 0)
    push_part = mm(moved, push, 1, 1)
    rows_part = sum(dot(part, chosen, 1, 0) for part in halves(moved))
    below_ref[...] = moved[: 2 * couple, :width]
    rest_ref[...] = moved[2 * couple :, :width]
    up_ref[...] = push_part[: 2 * couple]
    turn_ref[...] = rows_part[: 2 * couple]
    down_ref[...] = rows_part[2 * couple : 3 * couple]
    push_base_ref[...] = push_part[3 * couple :]
    row_base_ref[...] = rows_part[3 * couple :]
    root_ref[:couple, :] = rows_part[couple : 2 * couple, :couple]
    root_ref[couple:, :] = rows_part[3 * couple :, :couple]


def project(top, *refs):
    state_ref, below_ref, moved_in_ref, lift_ref, pair_ref, above_ref, back_ref = refs[:7]
    below_map_ref, rest_ref, metric_ref, basis_leaf_ref, basis_sep_ref = refs[7:12]
    leaf_ref, sep_ref, inner_ref = refs[12:]
    couple = moved_in_ref.shape[1]
    block = state_ref.shape[0]
    rank = basis_leaf_ref.shape[0]
    level = level_of(lax.axis_index("leaf"), top)
    above = jnp.where(level == 1, below_ref[:, couple:], moved_in_ref[...])
    leaf = state_ref[...] - mm(above, lift_ref[...])
    width = sep_ref.shape[1]
    is_root = level > top
    upper = jnp.where(is_root, back_ref[...], pair_ref[:, couple:])
    around = jnp.concatenate([jnp.where(is_root, 0.0, pair_ref[:, :couple]), upper], 1)
    sep = (
        rest_ref[couple:, :width]
        - mm(around, below_map_ref[...])
        - mm(above_ref[...], rest_ref[:couple, :width])
    )
    leaf_ref[...] = leaf
    sep_ref[...] = sep
    row = lax.broadcasted_iota(jnp.int32, (block, block), 0)
    lane = lax.broadcasted_iota(jnp.int32, (block, block), 1)
    corner = metric_ref[:block, :block]
    length = mm(leaf, leaf, 1, 1) + mm(sep, sep, 1, 1)
    inner_ref[...] = jnp.zeros(inner_ref.shape, jnp.float32)
    inner_ref[:, :rank] = mm(leaf, basis_leaf_ref[...], 1, 1) + mm(sep, basis_sep_ref[...], 1, 1)
    inner_ref[:, rank : rank + block] = jnp.where(row <= lane, length, corner)
    place = rank + block
    inner_ref[:, place : place + 1] = jnp.sum(jnp.where(row == lane, corner, 0.0), 1, keepdims=True)
    rest = rank - block
    inner_ref[:, place + 1 : place + 1 + rest] = metric_ref[:block, block:]
    inner_ref[:rest, place + 1 + rest : place + 1 + 2 * rest] = metric_ref[block:, block:]


def finish(total_rows, inner_ref, leaf_ref, sep_ref, basis_leaf_ref, basis_sep_ref, *outs):
    q_leaf_ref, q_sep_ref, coeffs_ref, rfac_ref = outs
    block = leaf_ref.shape[0]
    rank = basis_leaf_ref.shape[0]
    rest = rank - block
    inner = jnp.sum(inner_ref[...], 0) * (1.0 / total_rows)
    row = lax.broadcasted_iota(jnp.int32, (block, block), 0)
    lane = lax.broadcasted_iota(jnp.int32, (block, block), 1)
    first = inner[:, :rank]
    both = inner[:, rank : rank + block]
    place = rank + block
    length = jnp.where(row <= lane, both, both.T)
    corner = jnp.where(row > lane, both, both.T)
    corner = jnp.where(row == lane, inner[:, place : place + 1], corner)
    side = inner[:, place + 1 : place + 1 + rest]
    last = inner[:rest, place + 1 + rest : place + 1 + 2 * rest]

    def by_metric(value):
        low, high = value[:, :block], value[:, block:]
        return jnp.concatenate(
            [mm(low, corner) + mm(high, side, 1, 1), mm(low, side) + mm(high, last)], 1
        )

    second = first - by_metric(first)
    third = second - by_metric(second)
    coeffs = first + second
    gram = length - mm(first, coeffs, 1, 1) - mm(second, second + third, 1, 1)
    coeffs_ref[...] = coeffs
    row = lax.broadcasted_iota(jnp.int32, (block, 2 * block), 0)
    lane = lax.broadcasted_iota(jnp.int32, (block, 2 * block), 1)
    table = jnp.concatenate([gram, (row == lane)[:, :block].astype(jnp.float32)], 1)
    pivots = jnp.ones((block, 2 * block), jnp.float32)
    width = 16
    for start in range(0, block, width):
        columns = [
            jnp.broadcast_to(table[:, k : k + 1], table.shape)
            for k in range(start, min(start + width, block))
        ]
        for place in range(len(columns)):
            k = start + place
            pivot = columns[place][k : k + 1, :]
            pivots = jnp.where(row == k, pivot, pivots)
            factor = jnp.where(row > k, columns[place] / pivot, 0.0)
            table = table - factor * table[k : k + 1, :]
            for later in range(place + 1, len(columns)):
                columns[later] = columns[later] - factor * columns[later][k : k + 1, :]
    table = table / jnp.sqrt(pivots)
    rfac_ref[...] = jnp.where(row <= lane, table, 0.0)[:, :block]
    back = table[:, block:]
    spread = mm(back, coeffs)
    q_leaf_ref[...] = mm(back, leaf_ref[...]) - mm(spread, basis_leaf_ref[...])
    q_sep_ref[...] = mm(back, sep_ref[...]) - mm(spread, basis_sep_ref[...])


def on_device(
    rhs_leaf,
    rhs_sep,
    inv_leaf,
    inv_sep,
    push_leaf,
    push_sep,
    pull_leaf,
    pull_sep,
    rows_leaf,
    rows_sep,
    pivot_leaf,
    pivot_sep,
    basis_leaf,
    basis_sep,
):
    group = lax.axis_index("leaf")
    groups = lax.axis_size("leaf")
    top = groups.bit_length() - 1
    leaf_rows = pivot_leaf.shape[1]
    sep_rows = pivot_sep.shape[1]
    leaf_width = rhs_leaf.shape[1]
    sep_width = rhs_sep.shape[1]
    couple = rows_leaf.shape[1]
    total_rows = groups * (leaf_rows + sep_rows)
    level = level_of(group, top)

    bulk = pl.pallas_call(
        pack,
        out_shape=pltpu.VMEM((sep_rows + 2 * couple + rhs_sep.shape[0], sep_width), jnp.float32),
        in_specs=[pl.BlockSpec(memory_space=pltpu.VMEM)] * 4,
        out_specs=pl.BlockSpec(memory_space=pltpu.VMEM),
        name="pack",
    )(inv_sep[0], push_sep[0], pull_sep[0], rhs_sep)
    first_rhs, bulk = lax.optimization_barrier((rhs_leaf, bulk))
    leaf_pieces = gathered_pieces(first_rhs, "front")
    bulk = doubled_pieces(bulk, "front")

    lists = jnp.concatenate([rows_leaf, rows_sep], 0)
    lists = lax.all_to_all(
        jnp.broadcast_to(lists[None], (groups,) + lists.shape), "leaf", 0, 0
    )
    vmem = pl.BlockSpec(memory_space=pltpu.VMEM)
    block = rhs_sep.shape[0]
    leaf_state, leaf_push = pl.pallas_call(
        solve_leaf,
        out_shape=(
            pltpu.VMEM((block, leaf_width), jnp.float32),
            pltpu.VMEM((block, couple), jnp.float32),
        ),
        in_specs=[vmem] * (3 + len(leaf_pieces)),
        out_specs=(vmem,) * 2,
        name="solve_leaf",
    )(pivot_leaf, inv_leaf[0], push_leaf[0], leaf_pieces[0], *held(leaf_pieces[1:]))
    leaf_push = summed_pairwise(gathered_pieces(leaf_push, "front"))

    shapes = (
        (2 * couple, sep_width),
        (couple + block, sep_width),
        (2 * couple, couple),
        (2 * couple, 2 * couple),
        (couple, 2 * couple),
        (block, couple),
        (block, 2 * couple),
        (couple + block, couple),
    )
    (
        below_map,
        rest,
        up_weights,
        turn_weights,
        down_weights,
        push_base,
        row_base,
        root_op,
    ) = pl.pallas_call(
        lambda *refs: reduce_front(top, *refs),
        out_shape=tuple(pltpu.VMEM(shape, jnp.float32) for shape in shapes),
        in_specs=[vmem] * (2 + len(bulk)),
        out_specs=(vmem,) * len(shapes),
        name="reduce_front",
    )(
        pivot_sep,
        *held([lists.reshape(2 * groups, couple)]),
        *[piece if k % 2 == 0 else held([piece])[0] for k, piece in enumerate(bulk)],
    )

    pull_pieces = doubled_pieces(pull_leaf[0], "front")
    leaf_turned = pl.pallas_call(
        turn_pull,
        out_shape=pltpu.VMEM((couple, leaf_rows), jnp.float32),
        in_specs=[vmem] * (1 + len(pull_pieces)),
        out_specs=vmem,
        name="turn_pull",
    )(pivot_leaf, pull_pieces[0], *held(pull_pieces[1:]))
    leaf_lift = mm(leaf_turned, inv_leaf[0], 1, 1)

    half = groups // 2
    root_op = swap(root_op, "leaf", half)

    pair = jnp.concatenate([swap(leaf_push, "leaf", 1), leaf_push], 1)
    pair = jnp.where(level == 1, pair, 0.0)
    for height in range(2, top + 1):
        step = 2 ** (height - 2)
        term = push_base - mm(pair, up_weights)
        upper = swap(term, "leaf", step)
        lower = swap(term, "leaf", 3 * step)
        pair = jnp.where(level == height, jnp.concatenate([lower, upper], 1), pair)

    term = push_base - mm(pair, up_weights)
    above = jnp.where(level == top, root_op[couple:] - mm(term, root_op[:couple]), 0.0)
    back = swap(term, "leaf", half)

    row_base = row_base - mm(pair, turn_weights)
    for height in range(top, 1, -1):
        step = 2 ** (height - 2)
        below = row_base - mm(above, down_weights)
        upper = swap(below[:, couple:], "leaf", step)
        lower = swap(below[:, :couple], "leaf", 3 * step)
        is_upper = (group // (2 * step)) % 2 == 1
        above = jnp.where(level == height - 1, jnp.where(is_upper, upper, lower), above)
    below = row_base - mm(above, down_weights)
    moved_in = swap(below[:, :couple], "leaf", 1)
    rank = basis_leaf.shape[0]
    metric = mm(basis_leaf, basis_leaf, 1, 1) + mm(basis_sep, basis_sep, 1, 1)
    lanes = -(-(3 * rank - block + 1) // 128) * 128
    leaf_solution, sep_solution, inner = pl.pallas_call(
        lambda *refs: project(top, *refs),
        out_shape=(
            pltpu.VMEM((block, leaf_width), jnp.float32),
            pltpu.VMEM((block, sep_width), jnp.float32),
            pltpu.VMEM((block, lanes), jnp.float32),
        ),
        in_specs=[vmem] * 12,
        out_specs=(vmem,) * 3,
        name="project",
    )(
        *held([leaf_state, below, moved_in, leaf_lift, pair, above, back, below_map, rest, metric]),
        basis_leaf,
        basis_sep,
    )
    inner = summed_pairwise(gathered_pieces(inner, "front"))
    inner = lax.all_to_all(
        jnp.broadcast_to(inner[None], (groups,) + inner.shape), "leaf", 0, 0
    )
    q_leaf, q_sep, coeffs, rfac = pl.pallas_call(
        lambda *refs: finish(total_rows, *refs),
        out_shape=(
            jax.ShapeDtypeStruct((block, leaf_width), jnp.float32),
            jax.ShapeDtypeStruct((block, sep_width), jnp.float32),
            jax.ShapeDtypeStruct((block, rank), jnp.float32),
            jax.ShapeDtypeStruct((block, block), jnp.float32),
        ),
        in_specs=[vmem] * 5,
        name="finish",
    )(*held([inner, leaf_solution, sep_solution]), basis_leaf, basis_sep)
    return q_leaf, q_sep, coeffs.T, rfac


def solution(mesh):
    placed = (
        P(None, ("leaf", "front")),
        P(None, ("leaf", "front")),
        P("leaf", "front", None),
        P("leaf", "front", None),
        P("leaf", None, "front"),
        P("leaf", None, "front"),
        P("leaf", "front", None),
        P("leaf", "front", None),
        P("leaf", None),
        P("leaf", None),
        P("leaf", None),
        P("leaf", None),
        P(None, ("leaf", "front")),
        P(None, ("leaf", "front")),
    )

    return jax.shard_map(
        on_device,
        mesh=mesh,
        in_specs=placed,
        out_specs=(P(None, ("leaf", "front")), P(None, ("leaf", "front")), P(), P()),
        check_vma=False,
    )
```

```python
import jax
import jax.numpy as jnp
from jax import lax
from jax.experimental import pallas as pl
from jax.experimental.pallas import tpu as pltpu
from jax.sharding import PartitionSpec as P


exact_mode = lax.Precision.HIGHEST


def mm(former, latter, left=1, right=0):
    return lax.dot_general(
        former,
        latter,
        (((left,), (right,)), ((), ())),
        precision=exact_mode,
        preferred_element_type=jnp.float32,
    )


def swap(value, axis, mask):
    count = lax.axis_size(axis)
    return lax.ppermute(value, axis, [(one, one ^ mask) for one in range(count)])


def gathered_pieces(value, axis):
    pieces = [value]
    count = lax.axis_size(axis)
    for mask in range(1, count):
        pieces.append(swap(value, axis, mask))
    return pieces


def doubled_pieces(value, axis):
    pieces = {0: value}
    mask = lax.axis_size(axis) // 2
    while mask:
        for k in sorted(pieces):
            pieces[k ^ mask] = swap(pieces[k], axis, mask)
        mask //= 2
    return [pieces[k] for k in sorted(pieces)]


def summed_pairwise(pieces):
    while len(pieces) > 1:
        pieces = [pieces[k] + pieces[k + 1] for k in range(0, len(pieces), 2)]
    return pieces[0]


def local_place(index, width, own):
    if width & (width - 1) == 0:
        return jnp.bitwise_xor(index, own * width)
    return jnp.bitwise_xor(index // width, own) * width + index % width


def level_of(group, top):
    level = jnp.int32(top + 1)
    for bit in range(top, 0, -1):
        level = jnp.where(group % 2**bit != 0, jnp.int32(bit), level)
    return level


def held(arrays):
    return [pltpu.with_memory_space_constraint(array, pltpu.VMEM) for array in arrays]


def pack(inv_ref, push_ref, pull_ref, rhs_ref, out_ref):
    width = push_ref.shape[1]
    place = 0
    for column in range(0, inv_ref.shape[1], width):
        out_ref[place : place + width, :] = inv_ref[:, column : column + width]
        place += width
    for ref in (push_ref, pull_ref, rhs_ref):
        out_ref[place : place + ref.shape[0], :] = ref[...]
        place += ref.shape[0]


def halves(value):
    high = value.astype(jnp.bfloat16)
    rest = value - high.astype(jnp.float32)
    middle = rest.astype(jnp.bfloat16)
    return high, middle, (rest - middle.astype(jnp.float32)).astype(jnp.bfloat16)


def dot(former, latter, left, right):
    return lax.dot_general(
        former, latter, (((left,), (right,)), ((), ())), preferred_element_type=jnp.float32
    )


def permuting(pivot_ref, width):
    rows = pivot_ref.shape[1]
    places = local_place(pivot_ref[...], width, lax.axis_index("front"))
    entry = lax.broadcasted_iota(jnp.int32, (rows, rows), 0)
    return (entry == places).astype(jnp.float32).astype(jnp.bfloat16)


def solve_leaf(pivot_ref, inv_ref, push_ref, *refs):
    pieces, (state_ref, term_ref) = refs[:-2], refs[-2:]
    hot = permuting(pivot_ref, pieces[0].shape[1])
    rhs = jnp.concatenate([piece[...] for piece in pieces], 1)
    block = rhs.shape[0]
    turned = dot(jnp.concatenate(halves(rhs), 0), hot, 1, 0)
    turned = turned[:block] + turned[block : 2 * block] + turned[2 * block :]
    state = mm(turned, inv_ref[...], 1, 1)
    state_ref[...] = state
    term_ref[...] = mm(state, push_ref[...], 1, 1)


def turn_pull(pivot_ref, *refs):
    pieces, turned_ref = refs[:-1], refs[-1]
    hot = permuting(pivot_ref, pieces[0].shape[0])
    pull = jnp.concatenate([piece[...] for piece in pieces], 0).T
    couple = pull.shape[0]
    turned = dot(jnp.concatenate(halves(pull), 0), hot, 1, 0)
    turned_ref[...] = turned[:couple] + turned[couple : 2 * couple] + turned[2 * couple :]


def reduce_front(top, pivot_ref, lists_ref, *refs):
    pieces = refs[:-8]
    below_ref, rest_ref, up_ref, turn_ref, down_ref, push_base_ref, row_base_ref, root_ref = refs[-8:]
    rows = pivot_ref.shape[1]
    width = pieces[0].shape[1]
    couple = lists_ref.shape[1]
    hot = permuting(pivot_ref, width)
    group = lax.axis_index("leaf")
    level = level_of(group, top)
    reach = jnp.where(level == 1, 0, jnp.left_shift(1, jnp.maximum(level - 2, 0)))
    lower = jnp.where(level == 1, group - 1, jnp.where(level > top, reach, group - reach))
    kind = jnp.where(level == 1, 0, 1)
    children = jnp.concatenate(
        [lists_ref[pl.ds(2 * child + kind, 1), :] for child in (lower, group + reach)], 1
    )
    children = local_place(children, width, lax.axis_index("front"))
    entry = lax.broadcasted_iota(jnp.int32, (rows, 2 * couple), 0)
    chosen = (entry == children).astype(jnp.float32).astype(jnp.bfloat16)
    mapped = []
    for piece in pieces:
        inverse = jnp.concatenate(
            [piece[place : place + width, :] for place in range(0, rows, width)], 1
        )
        mapped.append(sum(dot(hot, part, 1, 1) for part in halves(inverse)))
    mapped = jnp.concatenate(mapped, 1)
    push = jnp.concatenate([piece[rows : rows + couple, :] for piece in pieces], 1)
    pull = jnp.concatenate([piece[rows + couple : rows + couple + width, :] for piece in pieces], 0)
    rhs = jnp.concatenate([piece[rows + couple + width :, :] for piece in pieces], 1)
    below = sum(dot(chosen, part, 0, 0) for part in halves(mapped))
    moved = jnp.concatenate([below, mm(jnp.concatenate([pull.T, rhs], 0), mapped)], 0)
    push_part = mm(moved, push, 1, 1)
    rows_part = sum(dot(part, chosen, 1, 0) for part in halves(moved))
    below_ref[...] = moved[: 2 * couple, :width]
    rest_ref[...] = moved[2 * couple :, :width]
    up_ref[...] = push_part[: 2 * couple]
    turn_ref[...] = rows_part[: 2 * couple]
    down_ref[...] = rows_part[2 * couple : 3 * couple]
    push_base_ref[...] = push_part[3 * couple :]
    row_base_ref[...] = rows_part[3 * couple :]
    root_ref[:couple, :] = rows_part[couple : 2 * couple, :couple]
    root_ref[couple:, :] = rows_part[3 * couple :, :couple]


def project(top, *refs):
    state_ref, leaf_above_ref, lift_ref, pair_ref, above_ref, back_ref = refs[:6]
    below_map_ref, rest_ref, metric_ref, basis_leaf_ref, basis_sep_ref = refs[6:11]
    leaf_ref, sep_ref, inner_ref = refs[11:]
    couple = leaf_above_ref.shape[1]
    block = state_ref.shape[0]
    rank = basis_leaf_ref.shape[0]
    level = level_of(lax.axis_index("leaf"), top)
    leaf = state_ref[...] - mm(leaf_above_ref[...], lift_ref[...])
    width = sep_ref.shape[1]
    is_root = level > top
    upper = jnp.where(is_root, back_ref[...], pair_ref[:, couple:])
    around = jnp.concatenate([jnp.where(is_root, 0.0, pair_ref[:, :couple]), upper], 1)
    sep = (
        rest_ref[couple:, :width]
        - mm(around, below_map_ref[...])
        - mm(above_ref[...], rest_ref[:couple, :width])
    )
    leaf_ref[...] = leaf
    sep_ref[...] = sep
    row = lax.broadcasted_iota(jnp.int32, (block, block), 0)
    lane = lax.broadcasted_iota(jnp.int32, (block, block), 1)
    corner = metric_ref[:block, :block]
    length = mm(leaf, leaf, 1, 1) + mm(sep, sep, 1, 1)
    inner_ref[...] = jnp.zeros(inner_ref.shape, jnp.float32)
    inner_ref[:, :rank] = mm(leaf, basis_leaf_ref[...], 1, 1) + mm(sep, basis_sep_ref[...], 1, 1)
    inner_ref[:, rank : rank + block] = jnp.where(row <= lane, length, corner)
    place = rank + block
    inner_ref[:, place : place + 1] = jnp.sum(jnp.where(row == lane, corner, 0.0), 1, keepdims=True)
    rest = rank - block
    inner_ref[:, place + 1 : place + 1 + rest] = metric_ref[:block, block:]
    inner_ref[:rest, place + 1 + rest : place + 1 + 2 * rest] = metric_ref[block:, block:]


def finish(total_rows, inner_ref, leaf_ref, sep_ref, basis_leaf_ref, basis_sep_ref, *outs):
    q_leaf_ref, q_sep_ref, coeffs_ref, rfac_ref = outs
    block = leaf_ref.shape[0]
    rank = basis_leaf_ref.shape[0]
    rest = rank - block
    inner = jnp.sum(inner_ref[...], 0) * (1.0 / total_rows)
    row = lax.broadcasted_iota(jnp.int32, (block, block), 0)
    lane = lax.broadcasted_iota(jnp.int32, (block, block), 1)
    first = inner[:, :rank]
    both = inner[:, rank : rank + block]
    place = rank + block
    length = jnp.where(row <= lane, both, both.T)
    corner = jnp.where(row > lane, both, both.T)
    corner = jnp.where(row == lane, inner[:, place : place + 1], corner)
    side = inner[:, place + 1 : place + 1 + rest]
    last = inner[:rest, place + 1 + rest : place + 1 + 2 * rest]

    def by_metric(value):
        low, high = value[:, :block], value[:, block:]
        return jnp.concatenate(
            [mm(low, corner) + mm(high, side, 1, 1), mm(low, side) + mm(high, last)], 1
        )

    second = first - by_metric(first)
    third = second - by_metric(second)
    coeffs = first + second
    gram = length - mm(first, coeffs, 1, 1) - mm(second, second + third, 1, 1)
    coeffs_ref[...] = coeffs
    row = lax.broadcasted_iota(jnp.int32, (block, 2 * block), 0)
    lane = lax.broadcasted_iota(jnp.int32, (block, 2 * block), 1)
    table = jnp.concatenate([gram, (row == lane)[:, :block].astype(jnp.float32)], 1)
    pivots = jnp.ones((block, 2 * block), jnp.float32)
    width = 16
    for start in range(0, block, width):
        columns = [
            jnp.broadcast_to(table[:, k : k + 1], table.shape)
            for k in range(start, min(start + width, block))
        ]
        for place in range(len(columns)):
            k = start + place
            pivot = columns[place][k : k + 1, :]
            pivots = jnp.where(row == k, pivot, pivots)
            factor = jnp.where(row > k, columns[place] / pivot, 0.0)
            table = table - factor * table[k : k + 1, :]
            for later in range(place + 1, len(columns)):
                columns[later] = columns[later] - factor * columns[later][k : k + 1, :]
    table = table / jnp.sqrt(pivots)
    rfac_ref[...] = jnp.where(row <= lane, table, 0.0)[:, :block]
    back = table[:, block:]
    spread = mm(back, coeffs)
    q_leaf_ref[...] = mm(back, leaf_ref[...]) - mm(spread, basis_leaf_ref[...])
    q_sep_ref[...] = mm(back, sep_ref[...]) - mm(spread, basis_sep_ref[...])


def on_device(
    rhs_leaf,
    rhs_sep,
    inv_leaf,
    inv_sep,
    push_leaf,
    push_sep,
    pull_leaf,
    pull_sep,
    rows_leaf,
    rows_sep,
    pivot_leaf,
    pivot_sep,
    basis_leaf,
    basis_sep,
):
    group = lax.axis_index("leaf")
    groups = lax.axis_size("leaf")
    top = groups.bit_length() - 1
    leaf_rows = pivot_leaf.shape[1]
    sep_rows = pivot_sep.shape[1]
    leaf_width = rhs_leaf.shape[1]
    sep_width = rhs_sep.shape[1]
    couple = rows_leaf.shape[1]
    total_rows = groups * (leaf_rows + sep_rows)
    level = level_of(group, top)

    bulk = pl.pallas_call(
        pack,
        out_shape=pltpu.VMEM((sep_rows + 2 * couple + rhs_sep.shape[0], sep_width), jnp.float32),
        in_specs=[pl.BlockSpec(memory_space=pltpu.VMEM)] * 4,
        out_specs=pl.BlockSpec(memory_space=pltpu.VMEM),
        name="pack",
    )(inv_sep[0], push_sep[0], pull_sep[0], rhs_sep)
    first_rhs, bulk = lax.optimization_barrier((rhs_leaf, bulk))
    leaf_pieces = gathered_pieces(first_rhs, "front")
    bulk = doubled_pieces(bulk, "front")

    lists = jnp.concatenate([rows_leaf, rows_sep], 0)
    lists = lax.all_to_all(
        jnp.broadcast_to(lists[None], (groups,) + lists.shape), "leaf", 0, 0
    )
    vmem = pl.BlockSpec(memory_space=pltpu.VMEM)
    block = rhs_sep.shape[0]
    leaf_state, leaf_push = pl.pallas_call(
        solve_leaf,
        out_shape=(
            pltpu.VMEM((block, leaf_width), jnp.float32),
            pltpu.VMEM((block, couple), jnp.float32),
        ),
        in_specs=[vmem] * (3 + len(leaf_pieces)),
        out_specs=(vmem,) * 2,
        name="solve_leaf",
    )(pivot_leaf, inv_leaf[0], push_leaf[0], leaf_pieces[0], *held(leaf_pieces[1:]))
    leaf_push = summed_pairwise(gathered_pieces(leaf_push, "front"))

    shapes = (
        (2 * couple, sep_width),
        (couple + block, sep_width),
        (2 * couple, couple),
        (2 * couple, 2 * couple),
        (couple, 2 * couple),
        (block, couple),
        (block, 2 * couple),
        (couple + block, couple),
    )
    (
        below_map,
        rest,
        up_weights,
        turn_weights,
        down_weights,
        push_base,
        row_base,
        root_op,
    ) = pl.pallas_call(
        lambda *refs: reduce_front(top, *refs),
        out_shape=tuple(pltpu.VMEM(shape, jnp.float32) for shape in shapes),
        in_specs=[vmem] * (2 + len(bulk)),
        out_specs=(vmem,) * len(shapes),
        name="reduce_front",
    )(
        pivot_sep,
        *held([lists.reshape(2 * groups, couple)]),
        *[piece if k % 2 == 0 else held([piece])[0] for k, piece in enumerate(bulk)],
    )

    pull_pieces = doubled_pieces(pull_leaf[0], "front")
    leaf_turned = pl.pallas_call(
        turn_pull,
        out_shape=pltpu.VMEM((couple, leaf_rows), jnp.float32),
        in_specs=[vmem] * (1 + len(pull_pieces)),
        out_specs=vmem,
        name="turn_pull",
    )(pivot_leaf, pull_pieces[0], *held(pull_pieces[1:]))
    leaf_lift = mm(leaf_turned, inv_leaf[0], 1, 1)

    half = groups // 2
    root_op = swap(root_op, "leaf", half)

    pair = jnp.concatenate([swap(leaf_push, "leaf", 1), leaf_push], 1)
    pair = jnp.where(level == 1, pair, 0.0)
    gift = row_base[:, :couple] - mm(pair, turn_weights[:, :couple])
    gift = jnp.concatenate([down_weights[:, :couple], gift], 0)
    gift = swap(gift, "leaf", 1)
    for height in range(2, top + 1):
        step = 2 ** (height - 2)
        term = push_base - mm(pair, up_weights)
        upper = swap(term, "leaf", step)
        lower = swap(term, "leaf", 3 * step)
        pair = jnp.where(level == height, jnp.concatenate([lower, upper], 1), pair)

    term = push_base - mm(pair, up_weights)
    above = jnp.where(level == top, root_op[couple:] - mm(term, root_op[:couple]), 0.0)
    back = swap(term, "leaf", half)

    row_base = row_base - mm(pair, turn_weights)
    for height in range(top, 1, -1):
        step = 2 ** (height - 2)
        below = row_base - mm(above, down_weights)
        lower = swap(below[:, :couple], "leaf", 3 * step)
        upper = swap(below[:, couple:], "leaf", step)
        if height == 2:
            across = swap(below[:, :couple], "leaf", 2)
        is_upper = (group // (2 * step)) % 2 == 1
        above = jnp.where(level == height - 1, jnp.where(is_upper, upper, lower), above)
    odd = level == 1
    own_way = jnp.concatenate([down_weights[:, couple:], row_base[:, couple:]], 0)
    way = jnp.where(odd, own_way, gift)
    source = jnp.where(odd, above, jnp.where(level == 2, below[:, couple:], across))
    leaf_above = way[couple:] - mm(source, way[:couple])

    rank = basis_leaf.shape[0]
    metric = mm(basis_leaf, basis_leaf, 1, 1) + mm(basis_sep, basis_sep, 1, 1)
    lanes = -(-(3 * rank - block + 1) // 128) * 128
    leaf_solution, sep_solution, inner = pl.pallas_call(
        lambda *refs: project(top, *refs),
        out_shape=(
            pltpu.VMEM((block, leaf_width), jnp.float32),
            pltpu.VMEM((block, sep_width), jnp.float32),
            pltpu.VMEM((block, lanes), jnp.float32),
        ),
        in_specs=[vmem] * 11,
        out_specs=(vmem,) * 3,
        name="project",
    )(
        *held([leaf_state, leaf_above, leaf_lift, pair, above, back, below_map, rest, metric]),
        basis_leaf,
        basis_sep,
    )
    inner = summed_pairwise(gathered_pieces(inner, "front"))
    inner = lax.all_to_all(
        jnp.broadcast_to(inner[None], (groups,) + inner.shape), "leaf", 0, 0
    )
    q_leaf, q_sep, coeffs, rfac = pl.pallas_call(
        lambda *refs: finish(total_rows, *refs),
        out_shape=(
            jax.ShapeDtypeStruct((block, leaf_width), jnp.float32),
            jax.ShapeDtypeStruct((block, sep_width), jnp.float32),
            jax.ShapeDtypeStruct((block, rank), jnp.float32),
            jax.ShapeDtypeStruct((block, block), jnp.float32),
        ),
        in_specs=[vmem] * 5,
        name="finish",
    )(*held([inner, leaf_solution, sep_solution]), basis_leaf, basis_sep)
    return q_leaf, q_sep, coeffs.T, rfac


def solution(mesh):
    placed = (
        P(None, ("leaf", "front")),
        P(None, ("leaf", "front")),
        P("leaf", "front", None),
        P("leaf", "front", None),
        P("leaf", None, "front"),
        P("leaf", None, "front"),
        P("leaf", "front", None),
        P("leaf", "front", None),
        P("leaf", None),
        P("leaf", None),
        P("leaf", None),
        P("leaf", None),
        P(None, ("leaf", "front")),
        P(None, ("leaf", "front")),
    )

    return jax.shard_map(
        on_device,
        mesh=mesh,
        in_specs=placed,
        out_specs=(P(None, ("leaf", "front")), P(None, ("leaf", "front")), P(), P()),
        check_vma=False,
    )
```
